32 devices in a mesh: fsdp: 4 (over x, core), vocab: 8 (over z, y).
Axes of the slice: x: 2, y: 2, z: 4, core: 2. Of those that a mesh axis runs over, the one named last changes fastest.
Arguments:
- hidden_states: bfloat16 [512, 3072], P('fsdp', 'vocab'), may hold values from -512 to 512
- head: bfloat16 [3072, 16384], P('fsdp', 'vocab'), may hold values from -0.25259074 to 0.25259074
- labels: int32 [512], P('fsdp'), may hold values from 0 to 16383
Outputs:
- token_loss: float32 [512], P('fsdp')
- state_grad: bfloat16 [512, 3072], P('fsdp', 'vocab')
- head_grad: float32 [3072, 16384], P('fsdp', 'vocab')
The draws below stay inside these ranges and needn't reach their ends.
All inputs are finite; a program needn't handle non-finite values.
Results may differ from the reference program's by a relative error of at most 0.0034.
Values may be sent and summed in bfloat16 or wider, within the bound.
A program may use at most 128 MiB of HBM per device.

```python
import math
import jax
import jax.numpy as jnp
from jax import lax

D = 3072
TOK_DEV = 128
VOCAB = 16384
TOKENS = 512


def head_matrix(key):
    base = jax.random.fold_in(key, 11)
    noise_key, spread_key = jax.random.split(base)
    noise = jnp.clip(jax.random.normal(noise_key, (D, VOCAB), jnp.float32), -5.0, 5.0)
    spread = jnp.exp(jax.random.uniform(spread_key, (VOCAB,), jnp.float32, math.log(0.8), math.log(1.25)))
    ramp = jnp.exp(math.log(2.2) * jnp.arange(VOCAB, dtype=jnp.float32) / VOCAB)
    return noise * (spread * ramp)[None, :] / math.sqrt(D)


def draw_head(key, part):
    return head_matrix(key).astype(jnp.bfloat16)


def draw_hidden_states(key, part):
    base = jax.random.fold_in(key, 23)
    scale_key, value_key = jax.random.split(base, 2)
    scale = jnp.exp(jax.random.uniform(scale_key, (TOKENS, 1), jnp.float32, math.log(0.35), math.log(1.0)))
    values = jnp.clip(jax.random.normal(value_key, (TOKENS, D), jnp.float32), -5.0, 5.0) * scale
    return values.astype(jnp.bfloat16)


def set_ends(array, rng, least, high):
    place = [jax.random.randint(jax.random.fold_in(rng, axis), (), 0, length) for axis, length in enumerate(array.shape)]
    longest = array.shape.index(max(array.shape))
    neighbour = place[:longest] + [(place[longest] + 1) % array.shape[longest]] + place[longest + 1:]
    return array.at[tuple(place)].set(least).at[tuple(neighbour)].set(high)


def setup_inputs(seed: int = 0) -> dict:
    splits = jax.random.split(jax.random.key(seed), 4)
    return {
        "hidden_states": draw_hidden_states(jax.random.fold_in(splits[3], 71), 0),
        "head": draw_head(jax.random.fold_in(splits[3], 71), 0),
        "labels": set_ends(jax.random.randint(splits[2], (TOKENS,), 0, VOCAB), jax.random.fold_in(splits[2], 1), 0, VOCAB - 1).astype(jnp.int32),
    }


def reference(hidden_states, head, labels):
    groups = TOKENS // TOK_DEV
    states = hidden_states.reshape(groups, TOK_DEV, D)
    targets = labels.reshape(groups, TOK_DEV)
    columns = jnp.arange(VOCAB, dtype=jnp.int32)

    def one_group(grad_sum, pair):
        block, wanted = pair
        logits = jnp.dot(block, head, preferred_element_type=jnp.float32)
        peak = jnp.max(logits, axis=1)
        shifted = jnp.exp(logits - peak[:, None])
        total = jnp.sum(shifted, axis=1)
        hits = wanted[:, None] == columns[None, :]
        target = jnp.sum(jnp.where(hits, logits, jnp.float32(0.0)), axis=1)
        loss = jnp.log(total) + peak - target
        errors = (shifted / total[:, None] - hits.astype(jnp.float32)).astype(jnp.bfloat16)
        state_part = lax.dot_general(errors, head, (((1,), (1,)), ((), ())), preferred_element_type=jnp.float32)
        term = lax.dot_general(block, errors, (((0,), (0,)), ((), ())), preferred_element_type=jnp.float32)
        return grad_sum + term, (loss, state_part.astype(jnp.bfloat16))

    start = jnp.zeros((D, VOCAB), jnp.float32)
    head_grad, outputs = lax.scan(one_group, start, (states, targets))
    token_loss = outputs[0].reshape(TOKENS)
    state_grad = outputs[1].reshape(TOKENS, D)
    return (token_loss, state_grad, head_grad)
```

```python
import functools

import jax
import jax.numpy as jnp
from jax import lax
from jax.experimental import pallas as pl
from jax.experimental.pallas import tpu as pltpu
from jax.sharding import PartitionSpec as P

CORES = 2
MESH = pl.DeviceIdType.MESH
NT = (((1,), (1,)), ((), ()))


def tile_of(size):
    return 256 if size % 256 == 0 else 128


def kernel(nf, nv, x_ref, head_hbm, lab_ref, loss_ref, grad_ref, err_out, feat_out,
           head, first, feats, labs, part, sib, xrecv, stats, errs, stf, stb, recv2, outb, fin,
           loc_sem, f1_s, f1_r, f2_s, f2_r, lab_s, lab_r, d_s, d_r, x_s, x_r, t_s, t_r,
           e_s, e_r, g_s, g_r, q_s, q_r, o_s, o_r):
    f = lax.axis_index("fsdp")
    v = lax.axis_index("vocab")
    r = nv // nf
    nx = nf // CORES
    xi, c = f // CORES, lax.rem(f, CORES)
    other = f + 1 - 2 * c
    width = head.shape[1]
    half = width // CORES
    tokens = feats.shape[0]
    tc = tokens // nv
    tx = tokens // nx
    db = x_ref.shape[1]
    dl = feats.shape[1]

    def rcopy(src, dst, s, q, ff, vv):
        return pltpu.make_async_remote_copy(
            src_ref=src, dst_ref=dst, send_sem=s, recv_sem=q,
            device_id=(ff, vv), device_id_type=MESH)

    def rows(index, size):
        return pl.ds(pl.multiple_of(index * size, size), size)

    load = pltpu.make_async_copy(head_hbm, head, loc_sem.at[0])
    load.start()

    jm = lax.rem(v, r)
    for i in range(r):
        piece = x_ref.at[pl.ds(i * tc, tc)]
        tf, tv = v // r, r * f + i
        mine = (tf == f) & (tv == v)

        @pl.when(mine)
        def _():
            pltpu.make_async_copy(piece, first.at[jm], f1_r.at[jm]).start()

        @pl.when(jnp.logical_not(mine))
        def _():
            rcopy(piece, first.at[jm], f1_s.at[i], f1_r.at[jm], tf, tv).start()

    labcopy = rcopy(lab_ref, labs.at[c], lab_s, lab_r, other, v)
    labcopy.start()
    labs[c] = lab_ref[...]

    for j in range(r):
        pltpu.make_async_copy(first.at[j], first.at[j], f1_r.at[j]).wait()
    for j in range(r):
        feats[rows(v, tc), j * db:(j + 1) * db] = first[j]
    gathers = []
    for d in range(1, nv):
        tv = lax.rem(v + d, nv)
        cp = rcopy(feats.at[rows(v, tc)], feats.at[rows(v, tc)], f2_s.at[d], f2_r.at[d], f, tv)
        cp.start()
        gathers.append(cp)
    load.wait()
    for d in range(1, nv):
        sv = lax.rem(v + nv - d, nv)
        pltpu.make_async_copy(feats.at[rows(sv, tc)], feats.at[rows(sv, tc)], f2_r.at[d]).wait()

    nt = tile_of(half)

    def logits_half(h):
        def tile(t, carry):
            col = pl.multiple_of(h * half + t * nt, nt)
            out = pl.multiple_of(t * nt, nt)
            part[h, :, pl.ds(out, nt)] = jnp.dot(
                feats[...], head[:, pl.ds(col, nt)], preferred_element_type=jnp.float32)
            return carry
        lax.fori_loop(0, half // nt, tile, 0)

    logits_half(1 - c)
    for d in list(range(1, nx)) + [0]:
        g = lax.rem(xi + d, nx)
        rcopy(part.at[1 - c, rows(g, tx)], sib.at[rows(g, tx)], d_s.at[d], d_r.at[d], other, v).start()
    logits_half(c)
    for d in list(range(1, nx)) + [0]:
        g = lax.rem(xi + d, nx)
        pltpu.make_async_copy(sib.at[rows(g, tx)], sib.at[rows(g, tx)], d_r.at[d]).wait()
        part[c, rows(g, tx)] = part[c, rows(g, tx)] + sib[rows(g, tx)]
        if d:
            rcopy(part.at[c, rows(g, tx)], xrecv.at[d - 1], x_s.at[d], x_r.at[d], g * CORES + c, v).start()

    outfeat = pltpu.make_async_copy(feats, feat_out, loc_sem.at[1])
    outfeat.start()

    labcopy.wait_recv()
    row = jnp.concatenate([labs[k] for k in range(CORES)], axis=1).astype(jnp.float32)
    want = jnp.broadcast_to(row, (128, tx)).T[:, :1]
    iota = lax.broadcasted_iota(jnp.int32, (tx, half), 1).astype(jnp.float32)
    base = (v * width + c * half).astype(jnp.float32)
    hits = (iota + base) == want

    for d in range(1, nx):
        pltpu.make_async_copy(xrecv.at[d - 1], xrecv.at[d - 1], x_r.at[d]).wait()
    logits = part[c, rows(xi, tx)]
    for d in range(1, nx):
        logits = logits + xrecv[d - 1]
    m = jnp.max(logits, axis=1, keepdims=True)
    shifted = jnp.exp(logits - m)
    s = jnp.sum(shifted, axis=1, keepdims=True)
    tg = jnp.sum(jnp.where(hits, logits, 0.0), axis=1, keepdims=True)
    lane = lax.broadcasted_iota(jnp.int32, (tx, 128), 1)
    packed = jnp.where(lane == 0, m, jnp.where(lane == 1, s, tg))
    me = v * CORES + c
    n = nv * CORES
    stats[me] = packed.T[:8]
    for d in range(1, n):
        to = lax.rem(me + d, n)
        rcopy(stats.at[me], stats.at[me], t_s.at[d], t_r.at[d],
              xi * CORES + lax.rem(to, CORES), to // CORES).start()
    for d in range(1, n):
        fr = lax.rem(me + n - d, n)
        pltpu.make_async_copy(stats.at[fr], stats.at[fr], t_r.at[d]).wait()
    peak = stats[0, 0:1]
    for k in range(1, n):
        peak = jnp.maximum(peak, stats[k, 0:1])
    total = jnp.zeros_like(peak)
    target = jnp.zeros_like(peak)
    for k in range(n):
        total = total + stats[k, 1:2] * jnp.exp(stats[k, 0:1] - peak)
        target = target + stats[k, 2:3]
    loss = jnp.log(total) + peak - target
    size = tx // CORES
    picked = loss[:, :size]
    for k in range(1, CORES):
        picked = jnp.where(c == k, loss[:, k * size:(k + 1) * size], picked)
    loss_ref[...] = picked
    sub = lax.broadcasted_iota(jnp.int32, (128, tx), 0)
    cols = jnp.where(sub == 0, peak, total).T
    scaled = jnp.exp(logits - cols[:, 0:1]) / cols[:, 1:2]
    errs[c, rows(xi, tx)] = (scaled - hits.astype(jnp.float32)).astype(jnp.bfloat16)

    mine = errs.at[c, rows(xi, tx)]
    for d in range(1, nx):
        g = lax.rem(xi + d, nx)
        rcopy(mine, mine, e_s.at[d], e_r.at[d], g * CORES + c, v).start()
    rcopy(mine, mine, g_s.at[0], g_r.at[0], other, v).start()
    for d in range(1, nx):
        g = lax.rem(xi + nx - d, nx)
        block = errs.at[c, rows(g, tx)]
        pltpu.make_async_copy(block, block, e_r.at[d]).wait()
        rcopy(block, block, g_s.at[d], g_r.at[d], other, v).start()
    for d in range(nx):
        g = lax.rem(xi + nx - d, nx)
        block = errs.at[1 - c, rows(g, tx)]
        pltpu.make_async_copy(block, block, g_r.at[d]).wait()
    outerr = []
    for h in range(CORES):
        cp = pltpu.make_async_copy(errs.at[h], err_out.at[:, pl.ds(h * half, half)], loc_sem.at[2 + h])
        cp.start()
        outerr.append(cp)

    dt = tile_of(dl)

    def state_tile(t, carry):
        at = pl.ds(pl.multiple_of(t * dt, dt), dt)
        acc = lax.dot_general(errs[0], head[at, 0:half], NT, preferred_element_type=jnp.float32)
        for h in range(1, CORES):
            acc = acc + lax.dot_general(
                errs[h], head[at, h * half:(h + 1) * half], NT, preferred_element_type=jnp.float32)
        stf[:, at] = acc
        stb[:, at] = acc.astype(jnp.bfloat16)
        return carry

    lax.fori_loop(0, dl // dt, state_tile, 0)
    for d in range(1, nv):
        tv = lax.rem(v + d, nv)
        rcopy(stb.at[rows(tv, tc)], recv2.at[d], q_s.at[d], q_r.at[d], f, tv).start()
    acc = stf[rows(v, tc), :]
    for d in range(1, nv):
        pltpu.make_async_copy(recv2.at[d], recv2.at[d], q_r.at[d]).wait()
        acc = acc + recv2[d].astype(jnp.float32)
    final = acc.astype(jnp.bfloat16)
    for j in range(r):
        outb[j] = final[:, j * db:(j + 1) * db]
    for j in range(r):
        tf, tv = v // r, r * f + j
        own = (tf == f) & (tv == v)

        @pl.when(own)
        def _():
            pltpu.make_async_copy(outb.at[j], fin.at[jm], o_r.at[jm]).start()

        @pl.when(jnp.logical_not(own))
        def _():
            rcopy(outb.at[j], fin.at[jm], o_s.at[j], o_r.at[jm], tf, tv).start()
    for j in range(r):
        pltpu.make_async_copy(fin.at[j], fin.at[j], o_r.at[j]).wait()
        grad_ref[j * tc:(j + 1) * tc, :] = fin[j]

    for i in range(r):
        own = (v // r == f) & (r * f + i == v)

        @pl.when(jnp.logical_not(own))
        def _():
            rcopy(x_ref.at[pl.ds(i * tc, tc)], first.at[jm], f1_s.at[i], f1_r.at[jm], v // r, r * f + i).wait_send()
            rcopy(outb.at[i], fin.at[jm], o_s.at[i], o_r.at[jm], v // r, r * f + i).wait_send()

    labcopy.wait_send()
    for cp in gathers:
        cp.wait_send()
    for d in range(nx):
        g = lax.rem(xi + d, nx)
        rcopy(part.at[1 - c, rows(g, tx)], sib.at[rows(g, tx)], d_s.at[d], d_r.at[d], other, v).wait_send()
        g2 = lax.rem(xi + nx - d, nx)
        block = errs.at[c, rows(g2, tx)]
        rcopy(block, block, g_s.at[d], g_r.at[d], other, v).wait_send()
        if d:
            rcopy(part.at[c, rows(g, tx)], xrecv.at[d - 1], x_s.at[d], x_r.at[d], g * CORES + c, v).wait_send()
            rcopy(mine_block(errs, c, rows(xi, tx)), mine_block(errs, c, rows(xi, tx)),
                  e_s.at[d], e_r.at[d], g * CORES + c, v).wait_send()
    for d in range(1, n):
        to = lax.rem(me + d, n)
        rcopy(stats.at[me], stats.at[me], t_s.at[d], t_r.at[d],
              xi * CORES + lax.rem(to, CORES), to // CORES).wait_send()
    for d in range(1, nv):
        tv = lax.rem(v + d, nv)
        rcopy(stb.at[rows(tv, tc)], recv2.at[d], q_s.at[d], q_r.at[d], f, tv).wait_send()
    outfeat.wait()
    for cp in outerr:
        cp.wait()


def mine_block(errs, c, where):
    return errs.at[c, where]


def local(nf, nv, hidden_states, head, labels):
    own, db = hidden_states.shape
    dl, width = head.shape
    tokens = own * nf
    half = width // CORES
    r, nx = nv // nf, nf // CORES
    tc, tx = tokens // nv, tokens // nx
    n = nv * CORES
    f32, bf16 = jnp.float32, jnp.bfloat16
    dma = pltpu.SemaphoreType.DMA
    vmem = pl.BlockSpec(memory_space=pltpu.VMEM)
    anyw = pl.BlockSpec(memory_space=pl.ANY)
    loss, grad, errors, feats = pl.pallas_call(
        functools.partial(kernel, nf, nv),
        out_shape=(
            jax.ShapeDtypeStruct((1, own), f32),
            jax.ShapeDtypeStruct((own, db), bf16),
            jax.ShapeDtypeStruct((tokens, width), bf16),
            jax.ShapeDtypeStruct((tokens, dl), bf16),
        ),
        in_specs=[vmem, anyw, vmem],
        out_specs=(vmem, vmem, anyw, anyw),
        scratch_shapes=[
            pltpu.VMEM((dl, width), bf16),
            pltpu.VMEM((r, tc, db), bf16),
            pltpu.VMEM((tokens, dl), bf16),
            pltpu.VMEM((CORES, 1, own), jnp.int32),
            pltpu.VMEM((CORES, tokens, half), f32),
            pltpu.VMEM((tokens, half), f32),
            pltpu.VMEM((max(nx - 1, 1), tx, half), f32),
            pltpu.VMEM((n, 8, tx), f32),
            pltpu.VMEM((CORES, tokens, half), bf16),
            pltpu.VMEM((tokens, dl), f32),
            pltpu.VMEM((tokens, dl), bf16),
            pltpu.VMEM((nv, tc, dl), bf16),
            pltpu.VMEM((r, tc, db), bf16),
            pltpu.VMEM((r, tc, db), bf16),
            dma((4,)), dma((r,)), dma((r,)), dma((nv,)), dma((nv,)), dma, dma,
            dma((nx,)), dma((nx,)), dma((nx,)), dma((nx,)), dma((n,)), dma((n,)),
            dma((nx,)), dma((nx,)), dma((nx,)), dma((nx,)), dma((nv,)), dma((nv,)),
            dma((r,)), dma((r,)),
        ],
        compiler_params=pltpu.CompilerParams(has_side_effects=True, vmem_limit_bytes=60 * 1024 * 1024),
    )(hidden_states, head, labels.reshape(1, own))
    head_grad = lax.dot_general(
        feats, errors, (((0,), (0,)), ((), ())), preferred_element_type=f32)
    return (loss.reshape(own), grad, head_grad)


def solution(mesh):
    sizes = dict(mesh.shape)
    body = functools.partial(local, sizes["fsdp"], sizes["vocab"])
    in_specs = (P("fsdp", "vocab"), P("fsdp", "vocab"), P("fsdp"))
    out_specs = (P("fsdp"), P("fsdp", "vocab"), P("fsdp", "vocab"))
    return jax.shard_map(body, mesh=mesh, in_specs=in_specs, out_specs=out_specs, check_vma=False)
```

```python
import functools

import jax
import jax.numpy as jnp
from jax import lax
from jax.experimental import pallas as pl
from jax.experimental.pallas import tpu as pltpu
from jax.sharding import PartitionSpec as P

CORES = 2
PAIR = 2
MESH = pl.DeviceIdType.MESH
NT = (((1,), (1,)), ((), ()))


def tile_of(size):
    return 256 if size % 256 == 0 else 128


def kernel(nf, nv, x_ref, head_hbm, lab_ref, loss_ref, grad_ref, err_out, feat_out,
           head, first, feats, labs, part, sib, xrecv, stats, errs, stf, stb, recv2, outb, fin,
           loc_sem, f1_s, f1_r, f2_s, f2_r, lab_s, lab_r, d_s, d_r, x_s, x_r, t_s, t_r,
           e_s, e_r, g_s, g_r, q_s, q_r, o_s, o_r):
    f = lax.axis_index("fsdp")
    v = lax.axis_index("vocab")
    r = nv // nf
    nx = nf // CORES
    xi, c = f // CORES, lax.rem(f, CORES)
    other = f + 1 - 2 * c
    width = head.shape[1]
    half = width // CORES
    tokens = feats.shape[0]
    tc = tokens // nv
    tx = tokens // nx
    db = x_ref.shape[1]
    dl = feats.shape[1]

    def rcopy(src, dst, s, q, ff, vv):
        return pltpu.make_async_remote_copy(
            src_ref=src, dst_ref=dst, send_sem=s, recv_sem=q,
            device_id=(ff, vv), device_id_type=MESH)

    def rows(index, size):
        return pl.ds(pl.multiple_of(index * size, size), size)

    load = pltpu.make_async_copy(head_hbm, head, loc_sem.at[0])
    load.start()

    jm = lax.rem(v, r)
    for i in range(r):
        piece = x_ref.at[pl.ds(i * tc, tc)]
        tf, tv = v // r, r * f + i
        mine = (tf == f) & (tv == v)

        @pl.when(mine)
        def _():
            pltpu.make_async_copy(piece, first.at[jm], f1_r.at[jm]).start()

        @pl.when(jnp.logical_not(mine))
        def _():
            rcopy(piece, first.at[jm], f1_s.at[i], f1_r.at[jm], tf, tv).start()

    labcopy = rcopy(lab_ref, labs.at[c], lab_s, lab_r, other, v)
    labcopy.start()
    labs[c] = lab_ref[...]

    for j in range(r):
        pltpu.make_async_copy(first.at[j], first.at[j], f1_r.at[j]).wait()
    for j in range(r):
        feats[rows(v, tc), j * db:(j + 1) * db] = first[j]
    na = nv // PAIR
    va, vb = v // PAIR, lax.rem(v, PAIR)
    pair = v + 1 - 2 * vb
    gathers = []

    def pass_on(index, d):
        cp = rcopy(feats.at[rows(index, tc)], feats.at[rows(index, tc)],
                   f2_s.at[na + d], f2_r.at[na + d], f, pair)
        cp.start()
        gathers.append(cp)

    for d in range(1, na):
        tv = lax.rem(va + d, na) * PAIR + vb
        cp = rcopy(feats.at[rows(v, tc)], feats.at[rows(v, tc)], f2_s.at[d], f2_r.at[d], f, tv)
        cp.start()
        gathers.append(cp)
    pass_on(v, 0)
    for d in range(1, na):
        sv = lax.rem(va + na - d, na) * PAIR + vb
        pltpu.make_async_copy(feats.at[rows(sv, tc)], feats.at[rows(sv, tc)], f2_r.at[d]).wait()
        pass_on(sv, d)
    load.wait()
    for d in range(na):
        sv = lax.rem(va + na - d, na) * PAIR + 1 - vb
        pltpu.make_async_copy(feats.at[rows(sv, tc)], feats.at[rows(sv, tc)], f2_r.at[na + d]).wait()

    nt = tile_of(half)

    def logits_part(g, h):
        def tile(t, carry):
            col = pl.multiple_of(h * half + t * nt, nt)
            out = pl.multiple_of(t * nt, nt)
            part[h, rows(g, tx), pl.ds(out, nt)] = jnp.dot(
                feats[rows(g, tx), :], head[:, pl.ds(col, nt)], preferred_element_type=jnp.float32)
            return carry
        lax.fori_loop(0, half // nt, tile, 0)

    def give(d):
        g = lax.rem(xi + d, nx)
        rcopy(part.at[1 - c, rows(g, tx)], sib.at[rows(g, tx)], d_s.at[d], d_r.at[d], other, v).start()

    def take(d):
        g = lax.rem(xi + d, nx)
        pltpu.make_async_copy(sib.at[rows(g, tx)], sib.at[rows(g, tx)], d_r.at[d]).wait()
        part[c, rows(g, tx)] = part[c, rows(g, tx)] + sib[rows(g, tx)]
        if d:
            rcopy(part.at[c, rows(g, tx)], xrecv.at[d - 1], x_s.at[d], x_r.at[d], g * CORES + c, v).start()

    for d in range(1, nx):
        logits_part(lax.rem(xi + d, nx), 1 - c)
        give(d)
        logits_part(lax.rem(xi + d, nx), c)
    for d in range(1, nx):
        take(d)
    logits_part(xi, 1 - c)
    give(0)
    logits_part(xi, c)
    take(0)

    outfeat = pltpu.make_async_copy(feats, feat_out, loc_sem.at[1])
    outfeat.start()

    labcopy.wait_recv()
    row = jnp.concatenate([labs[k] for k in range(CORES)], axis=1).astype(jnp.float32)
    want = jnp.broadcast_to(row, (128, tx)).T[:, :1]
    iota = lax.broadcasted_iota(jnp.int32, (tx, half), 1).astype(jnp.float32)
    base = (v * width + c * half).astype(jnp.float32)
    hits = (iota + base) == want

    for d in range(1, nx):
        pltpu.make_async_copy(xrecv.at[d - 1], xrecv.at[d - 1], x_r.at[d]).wait()
    logits = part[c, rows(xi, tx)]
    for d in range(1, nx):
        logits = logits + xrecv[d - 1]
    m = jnp.max(logits, axis=1, keepdims=True)
    shifted = jnp.exp(logits - m)
    s = jnp.sum(shifted, axis=1, keepdims=True)
    tg = jnp.sum(jnp.where(hits, logits, 0.0), axis=1, keepdims=True)
    lane = lax.broadcasted_iota(jnp.int32, (tx, 128), 1)
    packed = jnp.where(lane == 0, m, jnp.where(lane == 1, s, tg))
    me = v * CORES + c
    n = nv * CORES
    stats[me] = packed.T[:8]
    for d in range(1, n):
        to = lax.rem(me + d, n)
        rcopy(stats.at[me], stats.at[me], t_s.at[d], t_r.at[d],
              xi * CORES + lax.rem(to, CORES), to // CORES).start()
    for d in range(1, n):
        fr = lax.rem(me + n - d, n)
        pltpu.make_async_copy(stats.at[fr], stats.at[fr], t_r.at[d]).wait()
    peak = stats[0, 0:1]
    for k in range(1, n):
        peak = jnp.maximum(peak, stats[k, 0:1])
    total = jnp.zeros_like(peak)
    target = jnp.zeros_like(peak)
    for k in range(n):
        total = total + stats[k, 1:2] * jnp.exp(stats[k, 0:1] - peak)
        target = target + stats[k, 2:3]
    loss = jnp.log(total) + peak - target
    size = tx // CORES
    picked = loss[:, :size]
    for k in range(1, CORES):
        picked = jnp.where(c == k, loss[:, k * size:(k + 1) * size], picked)
    loss_ref[...] = picked
    sub = lax.broadcasted_iota(jnp.int32, (128, tx), 0)
    cols = jnp.where(sub == 0, peak, total).T
    scaled = jnp.exp(logits - cols[:, 0:1]) / cols[:, 1:2]
    errs[c, rows(xi, tx)] = (scaled - hits.astype(jnp.float32)).astype(jnp.bfloat16)

    mine = errs.at[c, rows(xi, tx)]
    for d in range(1, nx):
        g = lax.rem(xi + d, nx)
        rcopy(mine, mine, e_s.at[d], e_r.at[d], g * CORES + c, v).start()
    rcopy(mine, mine, g_s.at[0], g_r.at[0], other, v).start()
    for d in range(1, nx):
        g = lax.rem(xi + nx - d, nx)
        block = errs.at[c, rows(g, tx)]
        pltpu.make_async_copy(block, block, e_r.at[d]).wait()
        rcopy(block, block, g_s.at[d], g_r.at[d], other, v).start()
    for d in range(nx):
        g = lax.rem(xi + nx - d, nx)
        block = errs.at[1 - c, rows(g, tx)]
        pltpu.make_async_copy(block, block, g_r.at[d]).wait()
    outerr = []
    for h in range(CORES):
        cp = pltpu.make_async_copy(errs.at[h], err_out.at[:, pl.ds(h * half, half)], loc_sem.at[2 + h])
        cp.start()
        outerr.append(cp)

    dt = tile_of(dl)

    def state_tile(t, carry):
        at = pl.ds(pl.multiple_of(t * dt, dt), dt)
        acc = lax.dot_general(errs[0], head[at, 0:half], NT, preferred_element_type=jnp.float32)
        for h in range(1, CORES):
            acc = acc + lax.dot_general(
                errs[h], head[at, h * half:(h + 1) * half], NT, preferred_element_type=jnp.float32)
        stf[:, at] = acc
        stb[:, at] = acc.astype(jnp.bfloat16)
        return carry

    lax.fori_loop(0, dl // dt, state_tile, 0)
    for d in range(1, nv):
        tv = lax.rem(v + d, nv)
        rcopy(stb.at[rows(tv, tc)], recv2.at[d], q_s.at[d], q_r.at[d], f, tv).start()
    acc = stf[rows(v, tc), :]
    for d in range(1, nv):
        pltpu.make_async_copy(recv2.at[d], recv2.at[d], q_r.at[d]).wait()
        acc = acc + recv2[d].astype(jnp.float32)
    final = acc.astype(jnp.bfloat16)
    for j in range(r):
        outb[j] = final[:, j * db:(j + 1) * db]
    for j in range(r):
        tf, tv = v // r, r * f + j
        own = (tf == f) & (tv == v)

        @pl.when(own)
        def _():
            pltpu.make_async_copy(outb.at[j], fin.at[jm], o_r.at[jm]).start()

        @pl.when(jnp.logical_not(own))
        def _():
            rcopy(outb.at[j], fin.at[jm], o_s.at[j], o_r.at[jm], tf, tv).start()
    for j in range(r):
        pltpu.make_async_copy(fin.at[j], fin.at[j], o_r.at[j]).wait()
        grad_ref[j * tc:(j + 1) * tc, :] = fin[j]

    for i in range(r):
        own = (v // r == f) & (r * f + i == v)

        @pl.when(jnp.logical_not(own))
        def _():
            rcopy(x_ref.at[pl.ds(i * tc, tc)], first.at[jm], f1_s.at[i], f1_r.at[jm], v // r, r * f + i).wait_send()
            rcopy(outb.at[i], fin.at[jm], o_s.at[i], o_r.at[jm], v // r, r * f + i).wait_send()

    labcopy.wait_send()
    for cp in gathers:
        cp.wait_send()
    for d in range(nx):
        g = lax.rem(xi + d, nx)
        rcopy(part.at[1 - c, rows(g, tx)], sib.at[rows(g, tx)], d_s.at[d], d_r.at[d], other, v).wait_send()
        g2 = lax.rem(xi + nx - d, nx)
        block = errs.at[c, rows(g2, tx)]
        rcopy(block, block, g_s.at[d], g_r.at[d], other, v).wait_send()
        if d:
            rcopy(part.at[c, rows(g, tx)], xrecv.at[d - 1], x_s.at[d], x_r.at[d], g * CORES + c, v).wait_send()
            rcopy(mine_block(errs, c, rows(xi, tx)), mine_block(errs, c, rows(xi, tx)),
                  e_s.at[d], e_r.at[d], g * CORES + c, v).wait_send()
    for d in range(1, n):
        to = lax.rem(me + d, n)
        rcopy(stats.at[me], stats.at[me], t_s.at[d], t_r.at[d],
              xi * CORES + lax.rem(to, CORES), to // CORES).wait_send()
    for d in range(1, nv):
        tv = lax.rem(v + d, nv)
        rcopy(stb.at[rows(tv, tc)], recv2.at[d], q_s.at[d], q_r.at[d], f, tv).wait_send()
    outfeat.wait()
    for cp in outerr:
        cp.wait()


def mine_block(errs, c, where):
    return errs.at[c, where]


def local(nf, nv, hidden_states, head, labels):
    own, db = hidden_states.shape
    dl, width = head.shape
    tokens = own * nf
    half = width // CORES
    r, nx = nv // nf, nf // CORES
    tc, tx = tokens // nv, tokens // nx
    n = nv * CORES
    f32, bf16 = jnp.float32, jnp.bfloat16
    dma = pltpu.SemaphoreType.DMA
    vmem = pl.BlockSpec(memory_space=pltpu.VMEM)
    anyw = pl.BlockSpec(memory_space=pl.ANY)
    loss, grad, errors, feats = pl.pallas_call(
        functools.partial(kernel, nf, nv),
        out_shape=(
            jax.ShapeDtypeStruct((1, own), f32),
            jax.ShapeDtypeStruct((own, db), bf16),
            jax.ShapeDtypeStruct((tokens, width), bf16),
            jax.ShapeDtypeStruct((tokens, dl), bf16),
        ),
        in_specs=[vmem, anyw, vmem],
        out_specs=(vmem, vmem, anyw, anyw),
        scratch_shapes=[
            pltpu.VMEM((dl, width), bf16),
            pltpu.VMEM((r, tc, db), bf16),
            pltpu.VMEM((tokens, dl), bf16),
            pltpu.VMEM((CORES, 1, own), jnp.int32),
            pltpu.VMEM((CORES, tokens, half), f32),
            pltpu.VMEM((tokens, half), f32),
            pltpu.VMEM((max(nx - 1, 1), tx, half), f32),
            pltpu.VMEM((n, 8, tx), f32),
            pltpu.VMEM((CORES, tokens, half), bf16),
            pltpu.VMEM((tokens, dl), f32),
            pltpu.VMEM((tokens, dl), bf16),
            pltpu.VMEM((nv, tc, dl), bf16),
            pltpu.VMEM((r, tc, db), bf16),
            pltpu.VMEM((r, tc, db), bf16),
            dma((4,)), dma((r,)), dma((r,)), dma((nv,)), dma((nv,)), dma, dma,
            dma((nx,)), dma((nx,)), dma((nx,)), dma((nx,)), dma((n,)), dma((n,)),
            dma((nx,)), dma((nx,)), dma((nx,)), dma((nx,)), dma((nv,)), dma((nv,)),
            dma((r,)), dma((r,)),
        ],
        compiler_params=pltpu.CompilerParams(has_side_effects=True, vmem_limit_bytes=60 * 1024 * 1024),
    )(hidden_states, head, labels.reshape(1, own))
    head_grad = lax.dot_general(
        feats, errors, (((0,), (0,)), ((), ())), preferred_element_type=f32)
    return (loss.reshape(own), grad, head_grad)


def solution(mesh):
    sizes = dict(mesh.shape)
    body = functools.partial(local, sizes["fsdp"], sizes["vocab"])
    in_specs = (P("fsdp", "vocab"), P("fsdp", "vocab"), P("fsdp"))
    out_specs = (P("fsdp"), P("fsdp", "vocab"), P("fsdp", "vocab"))
    return jax.shard_map(body, mesh=mesh, in_specs=in_specs, out_specs=out_specs, check_vma=False)
```

```python
import functools

import jax
import jax.numpy as jnp
from jax import lax
from jax.experimental import pallas as pl
from jax.experimental.pallas import tpu as pltpu
from jax.sharding import PartitionSpec as P

CORES = 2
PAIR = 2
MESH = pl.DeviceIdType.MESH
NT = (((1,), (1,)), ((), ()))


def tile_of(size):
    return 256 if size % 256 == 0 else 128


def kernel(nf, nv, x_ref, head_hbm, lab_ref, loss_ref, grad_ref, err_out, feat_out,
           head, first, feats, labs, part, sib, xrecv, stats, errs, stf, stb, recv2, outb, fin,
           loc_sem, f1_s, f1_r, f2_s, f2_r, lab_s, lab_r, d_s, d_r, x_s, x_r, t_s, t_r,
           e_s, e_r, g_s, g_r, q_s, q_r, o_s, o_r):
    f = lax.axis_index("fsdp")
    v = lax.axis_index("vocab")
    r = nv // nf
    nx = nf // CORES
    xi, c = f // CORES, lax.rem(f, CORES)
    other = f + 1 - 2 * c
    width = head.shape[1]
    half = width // CORES
    tokens = feats.shape[0]
    tc = tokens // nv
    tx = tokens // nx
    db = x_ref.shape[1]
    dl = feats.shape[1]

    def rcopy(src, dst, s, q, ff, vv):
        return pltpu.make_async_remote_copy(
            src_ref=src, dst_ref=dst, send_sem=s, recv_sem=q,
            device_id=(ff, vv), device_id_type=MESH)

    def rows(index, size):
        return pl.ds(pl.multiple_of(index * size, size), size)

    load = pltpu.make_async_copy(head_hbm, head, loc_sem.at[0])
    load.start()

    jm = lax.rem(v, r)
    for i in range(r):
        piece = x_ref.at[pl.ds(i * tc, tc)]
        tf, tv = v // r, r * f + i
        mine = (tf == f) & (tv == v)

        @pl.when(mine)
        def _():
            pltpu.make_async_copy(piece, first.at[jm], f1_r.at[jm]).start()

        @pl.when(jnp.logical_not(mine))
        def _():
            rcopy(piece, first.at[jm], f1_s.at[i], f1_r.at[jm], tf, tv).start()

    labcopy = rcopy(lab_ref, labs.at[c], lab_s, lab_r, other, v)
    labcopy.start()
    labs[c] = lab_ref[...]

    for j in range(r):
        pltpu.make_async_copy(first.at[j], first.at[j], f1_r.at[j]).wait()
    for j in range(r):
        feats[rows(v, tc), j * db:(j + 1) * db] = first[j]
    na = nv // PAIR
    va, vb = v // PAIR, lax.rem(v, PAIR)
    pair = v + 1 - 2 * vb
    gathers = []

    def pass_on(index, d):
        cp = rcopy(feats.at[rows(index, tc)], feats.at[rows(index, tc)],
                   f2_s.at[na + d], f2_r.at[na + d], f, pair)
        cp.start()
        gathers.append(cp)

    for d in range(1, na):
        tv = lax.rem(va + d, na) * PAIR + vb
        cp = rcopy(feats.at[rows(v, tc)], feats.at[rows(v, tc)], f2_s.at[d], f2_r.at[d], f, tv)
        cp.start()
        gathers.append(cp)
    pass_on(v, 0)
    for d in range(1, na):
        sv = lax.rem(va + na - d, na) * PAIR + vb
        pltpu.make_async_copy(feats.at[rows(sv, tc)], feats.at[rows(sv, tc)], f2_r.at[d]).wait()
        pass_on(sv, d)
    load.wait()
    for d in range(na):
        sv = lax.rem(va + na - d, na) * PAIR + 1 - vb
        pltpu.make_async_copy(feats.at[rows(sv, tc)], feats.at[rows(sv, tc)], f2_r.at[na + d]).wait()

    nt = tile_of(half)

    def logits_part(g, h):
        def tile(t, carry):
            col = pl.multiple_of(h * half + t * nt, nt)
            out = pl.multiple_of(t * nt, nt)
            part[h, rows(g, tx), pl.ds(out, nt)] = jnp.dot(
                feats[rows(g, tx), :], head[:, pl.ds(col, nt)], preferred_element_type=jnp.float32)
            return carry
        lax.fori_loop(0, half // nt, tile, 0)

    def give(d):
        g = lax.rem(xi + d, nx)
        rcopy(part.at[1 - c, rows(g, tx)], sib.at[rows(g, tx)], d_s.at[d], d_r.at[d], other, v).start()

    def take(d):
        g = lax.rem(xi + d, nx)
        pltpu.make_async_copy(sib.at[rows(g, tx)], sib.at[rows(g, tx)], d_r.at[d]).wait()
        part[c, rows(g, tx)] = part[c, rows(g, tx)] + sib[rows(g, tx)]
        if d:
            rcopy(part.at[c, rows(g, tx)], xrecv.at[d - 1], x_s.at[d], x_r.at[d], g * CORES + c, v).start()

    for d in range(1, nx):
        logits_part(lax.rem(xi + d, nx), 1 - c)
        give(d)
        logits_part(lax.rem(xi + d, nx), c)
    for d in range(1, nx):
        take(d)
    logits_part(xi, 1 - c)
    give(0)
    logits_part(xi, c)
    take(0)

    outfeat = pltpu.make_async_copy(feats, feat_out, loc_sem.at[1])
    outfeat.start()

    labcopy.wait_recv()
    row = jnp.concatenate([labs[k] for k in range(CORES)], axis=1).astype(jnp.float32)
    want = jnp.broadcast_to(row, (128, tx)).T[:, :1]
    iota = lax.broadcasted_iota(jnp.int32, (tx, half), 1).astype(jnp.float32)
    base = (v * width + c * half).astype(jnp.float32)
    hits = (iota + base) == want

    for d in range(1, nx):
        pltpu.make_async_copy(xrecv.at[d - 1], xrecv.at[d - 1], x_r.at[d]).wait()
    logits = part[c, rows(xi, tx)]
    for d in range(1, nx):
        logits = logits + xrecv[d - 1]
    m = jnp.max(logits, axis=1, keepdims=True)
    shifted = jnp.exp(logits - m)
    s = jnp.sum(shifted, axis=1, keepdims=True)
    tg = jnp.sum(jnp.where(hits, logits, 0.0), axis=1, keepdims=True)
    lane = lax.broadcasted_iota(jnp.int32, (tx, 128), 1)
    packed = jnp.where(lane == 0, m, jnp.where(lane == 1, s, tg))
    me = v * CORES + c
    n = nv * CORES
    stats[me] = packed.T[:8]
    for d in range(1, n):
        to = lax.rem(me + d, n)
        rcopy(stats.at[me], stats.at[me], t_s.at[d], t_r.at[d],
              xi * CORES + lax.rem(to, CORES), to // CORES).start()
    for d in range(1, n):
        fr = lax.rem(me + n - d, n)
        pltpu.make_async_copy(stats.at[fr], stats.at[fr], t_r.at[d]).wait()
    peak = stats[0, 0:1]
    for k in range(1, n):
        peak = jnp.maximum(peak, stats[k, 0:1])
    total = jnp.zeros_like(peak)
    target = jnp.zeros_like(peak)
    for k in range(n):
        total = total + stats[k, 1:2] * jnp.exp(stats[k, 0:1] - peak)
        target = target + stats[k, 2:3]
    loss = jnp.log(total) + peak - target
    size = tx // CORES
    picked = loss[:, :size]
    for k in range(1, CORES):
        picked = jnp.where(c == k, loss[:, k * size:(k + 1) * size], picked)
    loss_ref[...] = picked
    sub = lax.broadcasted_iota(jnp.int32, (128, tx), 0)
    cols = jnp.where(sub == 0, peak, total).T
    scaled = jnp.exp(logits - cols[:, 0:1]) / cols[:, 1:2]
    errs[c, rows(xi, tx)] = (scaled - hits.astype(jnp.float32)).astype(jnp.bfloat16)

    mine = errs.at[c, rows(xi, tx)]
    for d in range(1, nx):
        g = lax.rem(xi + d, nx)
        rcopy(mine, mine, e_s.at[d], e_r.at[d], g * CORES + c, v).start()
    rcopy(mine, mine, g_s.at[0], g_r.at[0], other, v).start()

    dt = tile_of(dl)

    def state_part(g):
        def tile(t, carry):
            at = pl.ds(pl.multiple_of(t * dt, dt), dt)
            acc = lax.dot_general(
                errs[0, rows(g, tx)], head[at, 0:half], NT, preferred_element_type=jnp.float32)
            for h in range(1, CORES):
                acc = acc + lax.dot_general(
                    errs[h, rows(g, tx)], head[at, h * half:(h + 1) * half], NT,
                    preferred_element_type=jnp.float32)
            stf[rows(g, tx), at] = acc
            stb[rows(g, tx), at] = acc.astype(jnp.bfloat16)
            return carry
        lax.fori_loop(0, dl // dt, tile, 0)
        for d in range(1, nv):
            tv = lax.rem(v + d, nv)

            @pl.when(tv // (nv // nx) == g)
            def _():
                rcopy(stb.at[rows(tv, tc)], recv2.at[d], q_s.at[d], q_r.at[d], f, tv).start()

    for d in range(nx):
        g = lax.rem(xi + nx - d, nx)
        block = errs.at[c, rows(g, tx)]
        if d:
            pltpu.make_async_copy(block, block, e_r.at[d]).wait()
            rcopy(block, block, g_s.at[d], g_r.at[d], other, v).start()
        block = errs.at[1 - c, rows(g, tx)]
        pltpu.make_async_copy(block, block, g_r.at[d]).wait()
        state_part(g)
    outerr = []
    for h in range(CORES):
        cp = pltpu.make_async_copy(errs.at[h], err_out.at[:, pl.ds(h * half, half)], loc_sem.at[2 + h])
        cp.start()
        outerr.append(cp)
    acc = stf[rows(v, tc), :]
    for d in range(1, nv):
        pltpu.make_async_copy(recv2.at[d], recv2.at[d], q_r.at[d]).wait()
        acc = acc + recv2[d].astype(jnp.float32)
    final = acc.astype(jnp.bfloat16)
    for j in range(r):
        outb[j] = final[:, j * db:(j + 1) * db]
    for j in range(r):
        tf, tv = v // r, r * f + j
        own = (tf == f) & (tv == v)

        @pl.when(own)
        def _():
            pltpu.make_async_copy(outb.at[j], fin.at[jm], o_r.at[jm]).start()

        @pl.when(jnp.logical_not(own))
        def _():
            rcopy(outb.at[j], fin.at[jm], o_s.at[j], o_r.at[jm], tf, tv).start()
    for j in range(r):
        pltpu.make_async_copy(fin.at[j], fin.at[j], o_r.at[j]).wait()
        grad_ref[j * tc:(j + 1) * tc, :] = fin[j]

    for i in range(r):
        own = (v // r == f) & (r * f + i == v)

        @pl.when(jnp.logical_not(own))
        def _():
            rcopy(x_ref.at[pl.ds(i * tc, tc)], first.at[jm], f1_s.at[i], f1_r.at[jm], v // r, r * f + i).wait_send()
            rcopy(outb.at[i], fin.at[jm], o_s.at[i], o_r.at[jm], v // r, r * f + i).wait_send()

    labcopy.wait_send()
    for cp in gathers:
        cp.wait_send()
    for d in range(nx):
        g = lax.rem(xi + d, nx)
        rcopy(part.at[1 - c, rows(g, tx)], sib.at[rows(g, tx)], d_s.at[d], d_r.at[d], other, v).wait_send()
        g2 = lax.rem(xi + nx - d, nx)
        block = errs.at[c, rows(g2, tx)]
        rcopy(block, block, g_s.at[d], g_r.at[d], other, v).wait_send()
        if d:
            rcopy(part.at[c, rows(g, tx)], xrecv.at[d - 1], x_s.at[d], x_r.at[d], g * CORES + c, v).wait_send()
            rcopy(mine_block(errs, c, rows(xi, tx)), mine_block(errs, c, rows(xi, tx)),
                  e_s.at[d], e_r.at[d], g * CORES + c, v).wait_send()
    for d in range(1, n):
        to = lax.rem(me + d, n)
        rcopy(stats.at[me], stats.at[me], t_s.at[d], t_r.at[d],
              xi * CORES + lax.rem(to, CORES), to // CORES).wait_send()
    for d in range(1, nv):
        tv = lax.rem(v + d, nv)
        rcopy(stb.at[rows(tv, tc)], recv2.at[d], q_s.at[d], q_r.at[d], f, tv).wait_send()
    outfeat.wait()
    for cp in outerr:
        cp.wait()


def mine_block(errs, c, where):
    return errs.at[c, where]


def local(nf, nv, hidden_states, head, labels):
    own, db = hidden_states.shape
    dl, width = head.shape
    tokens = own * nf
    half = width // CORES
    r, nx = nv // nf, nf // CORES
    tc, tx = tokens // nv, tokens // nx
    n = nv * CORES
    f32, bf16 = jnp.float32, jnp.bfloat16
    dma = pltpu.SemaphoreType.DMA
    vmem = pl.BlockSpec(memory_space=pltpu.VMEM)
    anyw = pl.BlockSpec(memory_space=pl.ANY)
    loss, grad, errors, feats = pl.pallas_call(
        functools.partial(kernel, nf, nv),
        out_shape=(
            jax.ShapeDtypeStruct((1, own), f32),
            jax.ShapeDtypeStruct((own, db), bf16),
            jax.ShapeDtypeStruct((tokens, width), bf16),
            jax.ShapeDtypeStruct((tokens, dl), bf16),
        ),
        in_specs=[vmem, anyw, vmem],
        out_specs=(vmem, vmem, anyw, anyw),
        scratch_shapes=[
            pltpu.VMEM((dl, width), bf16),
            pltpu.VMEM((r, tc, db), bf16),
            pltpu.VMEM((tokens, dl), bf16),
            pltpu.VMEM((CORES, 1, own), jnp.int32),
            pltpu.VMEM((CORES, tokens, half), f32),
            pltpu.VMEM((tokens, half), f32),
            pltpu.VMEM((max(nx - 1, 1), tx, half), f32),
            pltpu.VMEM((n, 8, tx), f32),
            pltpu.VMEM((CORES, tokens, half), bf16),
            pltpu.VMEM((tokens, dl), f32),
            pltpu.VMEM((tokens, dl), bf16),
            pltpu.VMEM((nv, tc, dl), bf16),
            pltpu.VMEM((r, tc, db), bf16),
            pltpu.VMEM((r, tc, db), bf16),
            dma((4,)), dma((r,)), dma((r,)), dma((nv,)), dma((nv,)), dma, dma,
            dma((nx,)), dma((nx,)), dma((nx,)), dma((nx,)), dma((n,)), dma((n,)),
            dma((nx,)), dma((nx,)), dma((nx,)), dma((nx,)), dma((nv,)), dma((nv,)),
            dma((r,)), dma((r,)),
        ],
        compiler_params=pltpu.CompilerParams(has_side_effects=True, vmem_limit_bytes=60 * 1024 * 1024),
    )(hidden_states, head, labels.reshape(1, own))
    head_grad = lax.dot_general(
        feats, errors, (((0,), (0,)), ((), ())), preferred_element_type=f32)
    return (loss.reshape(own), grad, head_grad)


def solution(mesh):
    sizes = dict(mesh.shape)
    body = functools.partial(local, sizes["fsdp"], sizes["vocab"])
    in_specs = (P("fsdp", "vocab"), P("fsdp", "vocab"), P("fsdp"))
    out_specs = (P("fsdp"), P("fsdp", "vocab"), P("fsdp", "vocab"))
    return jax.shard_map(body, mesh=mesh, in_specs=in_specs, out_specs=out_specs, check_vma=False)
```
